256 devices in a mesh: series: 8 (over x_hi, y), tm: 32 (over z, x_lo, core).
Axes of the slice: x: 4 (x_hi: 2, x_lo: 2; x = x_hi * 2 + x_lo), y: 4, z: 8, core: 2. Of those that a mesh axis runs over, the one named last changes fastest.
Arguments:
- observed: bfloat16 [16384, 32768], P('series', 'tm'), may hold values from -6 to 6
- mask: bfloat16 [16384, 32768], P('series', 'tm'), may hold values from 0 to 1, as said below
- loadings: float32 [16384, 128], P('series'), may hold values from -0.5 to 0.5
- factors: float32 [32768, 128], P('tm'), may hold values from -6 to 6
- lag_weights: float32 [2, 128], replicated, may hold values from 0.2 to 0.7
Outputs:
- new_loadings: float32 [16384, 128], P('series')
- new_factors: float32 [32768, 128], P('tm')
The draws below stay inside these ranges and needn't reach their ends.
Inputs may be any that keep to these rules, and one draw needn't show every extreme that they name: `mask`: each entry is 0 or 1.
All inputs are finite; a program needn't handle non-finite values.
Results may differ from the reference program's by a relative error of at most 0.0041.
Values sent between devices are 32-bit elements; how exact they have to be, the bound alone decides.
A program may use at most 128 MiB of HBM per device.

```python
import jax
import jax.numpy as jnp
from jax import lax

RANK = 128
LAG = 1440
OUTER = 2
TIME_STEPS = 2
SERIES = 16384
MINUTES = 32768


def draw_mask(key, part):
    sample = jax.random.uniform(jax.random.fold_in(key, 17), (SERIES, MINUTES), jnp.float32)
    return jnp.where(sample < 0.7, 1.0, 0.0).astype(jnp.float32).astype(jnp.bfloat16)


def block_scale(rng, extent, pieces, low, top_value):
    level, own = 1.0, jax.random.fold_in(rng, 6)
    for axis_at, shards_of in pieces:
        draws = jnp.exp(jax.random.uniform(jax.random.fold_in(own, axis_at), (shards_of,), jnp.float32, low / len(pieces), top_value / len(pieces)))
        level = level * jnp.repeat(draws, extent[axis_at] // shards_of).reshape([-1 if axis == axis_at else 1 for axis in range(len(extent))])
    return level


def bell_draw(own_key, shape, spread, reach, pieces=(), held_as=jnp.bfloat16):
    drawn = jax.random.normal(own_key, shape, jnp.float32) * spread
    if len(pieces) > 0:
        drawn = block_scale(own_key, shape, pieces, -0.22, 0.18) * drawn
    return jnp.clip(drawn, min=-reach, max=reach).astype(held_as)


def setup_inputs(seed: int = 0) -> dict:
    splits = jax.random.split(jax.random.key(seed), 6)
    return {
        "observed": bell_draw(splits[0], (SERIES, MINUTES), 1.0, 6.0, ((0, 8), (1, 32))),
        "mask": draw_mask(jax.random.fold_in(splits[5], 71), 0),
        "loadings": bell_draw(splits[2], (SERIES, RANK), RANK ** -0.5, 0.5, ((0, 8),), jnp.float32),
        "factors": bell_draw(splits[3], (MINUTES, RANK), 1.0, 6.0, ((0, 32),), jnp.float32),
        "lag_weights": jnp.clip(jax.random.uniform(splits[4], (2, RANK), jnp.float32, 0.2, 0.7), 0.2, 0.7),
    }


smooth = 4.0
shrink = 0.1
margin = 32.0

def back(z, lag):
    return jnp.concatenate([jnp.zeros((lag, z.shape[1]), jnp.float32), z[:-lag]], axis=0)

def ahead(z, lag):
    return jnp.concatenate([z[lag:], jnp.zeros((lag, z.shape[1]), jnp.float32)], axis=0)

def block_residual(observed, mask, fb, xb):
    prod = lax.dot_general(fb, xb, (((1,), (1,)), ((), ())), preferred_element_type=jnp.float32)
    return (mask.astype(jnp.float32) * (prod - observed.astype(jnp.float32))).astype(jnp.bfloat16)

def reference(observed, mask, loadings, factors, lag_weights):
    step_time = 1.0 / (SERIES / RANK + margin)
    step_load = 1.0 / MINUTES
    block = min(2048, SERIES)
    count = SERIES // block
    obs_blocks = observed.reshape(count, block, MINUTES)
    mask_blocks = mask.reshape(count, block, MINUTES)
    loads = loadings
    times = factors
    for outer in range(OUTER):
        for inner in range(TIME_STEPS):
            fb = loads.astype(jnp.bfloat16).reshape(count, block, RANK)
            xb = times.astype(jnp.bfloat16)

            def accumulate(total, items):
                obs_b, mask_b, fb_b = items
                rb = block_residual(obs_b, mask_b, fb_b, xb)
                return (total + lax.dot_general(rb, fb_b, (((0,), (0,)), ((), ())), preferred_element_type=jnp.float32), None)
            grad, unused = lax.scan(accumulate, jnp.zeros((MINUTES, RANK), jnp.float32), (obs_blocks, mask_blocks, fb))
            resid = times - lag_weights[0] * back(times, 1) - lag_weights[1] * back(times, LAG)
            smooth_grad = smooth * (resid - lag_weights[0] * ahead(resid, 1) - lag_weights[1] * ahead(resid, LAG))
            times = times - step_time * (grad + smooth_grad)
        fb = loads.astype(jnp.bfloat16).reshape(count, block, RANK)
        xb = times.astype(jnp.bfloat16)

        def loading_grad(items):
            obs_b, mask_b, fb_b = items
            rb = block_residual(obs_b, mask_b, fb_b, xb)
            return jnp.dot(rb, xb, preferred_element_type=jnp.float32)
        grad_f = lax.map(loading_grad, (obs_blocks, mask_blocks, fb)).reshape(SERIES, RANK)
        loads = loads - step_load * (grad_f + shrink * loads)
    return (loads, times)
```

```python
import functools

import jax
import jax.numpy as jnp
from jax import lax
from jax.experimental import pallas as pl
from jax.experimental.pallas import tpu as pltpu
from jax.sharding import PartitionSpec as P

LAG = 1440
OUTER = 2
TIME_STEPS = 2
STEPS = OUTER * TIME_STEPS
CHUNKS = 4

smooth = 4.0
shrink = 0.1
margin = 32.0

MESH = pl.DeviceIdType.MESH
F32 = jnp.float32
BF16 = jnp.bfloat16
NT = (((1,), (1,)), ((), ()))


def rows_of(start, size):
    return pl.ds(pl.multiple_of(start, size), size)


def kernel(
    groups, spans,
    obs_hbm, mask_hbm, loads_hbm, times_hbm, weights,
    loads_out, times_out,
    obs, mask, fs, xs, gs, hs, got_g, got_h, core_h, sum_h,
    back, ahead, edge_before, edge_after,
    fb, fbt, xb, resid, resid_f, window,
    in_sem, tile_sem, out_sem,
    g_send, g_recv, x_send, x_recv,
    halo_send, back_recv, ahead_recv, edge_recv,
    core_send, core_recv, h_send, h_recv, f_send, f_recv, pair_send, pair_recv,
):
    n_series, n_tm = groups
    series, minutes = spans
    rank = weights.shape[1]
    n_pair = n_tm // 2
    cols = minutes // CHUNKS
    own = cols // n_series
    granules = minutes // own
    far = LAG // own
    far_in = far % granules
    series_rows = series // CHUNKS
    half = series_rows // 2
    own_f = half // n_pair
    total_minutes = minutes * n_tm
    step_time = 1.0 / (series * n_series / rank + margin)
    step_load = 1.0 / total_minutes

    s = lax.axis_index("series")
    m = lax.axis_index("tm")
    core = lax.rem(m, 2)
    pair = m // 2
    partner = m + 1 - 2 * core

    def send(src, dst, send_sem, recv_sem, to_s, to_m):
        pltpu.make_async_remote_copy(
            src_ref=src, dst_ref=dst, send_sem=send_sem, recv_sem=recv_sem,
            device_id=(to_s, to_m), device_id_type=MESH,
        ).start()

    def wait_for(ref, sem):
        pltpu.make_async_copy(ref, ref, sem).wait()

    barrier = pltpu.get_barrier_semaphore()

    def greet(to_s, to_m):
        pl.semaphore_signal(barrier, inc=1, device_id=(to_s, to_m), device_id_type=MESH)

    for d in range(1, n_series):
        greet(lax.rem(s + d, n_series), m)
    for d in range(1, n_pair):
        greet(s, 2 * lax.rem(pair + d, n_pair) + core)
    greet(s, partner)
    greet(s, lax.rem(m + 1, n_tm))
    greet(s, lax.rem(m + n_tm - 1, n_tm))
    greetings = (n_series - 1) + (n_pair - 1) + 3

    times_in = pltpu.make_async_copy(times_hbm, xs.at[0], in_sem.at[0])
    loads_in = pltpu.make_async_copy(loads_hbm, fs.at[0], in_sem.at[1])
    times_in.start()
    loads_in.start()

    def tile_in(c, which):
        ref, hbm = ((obs, obs_hbm), (mask, mask_hbm))[which]
        at = rows_of(c * cols, cols)
        return pltpu.make_async_copy(hbm.at[:, at], ref.at[:, at], tile_sem.at[which, c])

    for c in range(CHUNKS):
        tile_in(c, 0).start()
        tile_in(c, 1).start()

    def halo_out(k, c):
        def place(offset, shift):
            g = c * n_series + lax.rem(s + offset, n_series)
            j = lax.rem(g + shift, granules)
            return g, j // n_series, (g + shift) // granules

        g, chunk, over = place(2 * n_series - far_in, far_in)
        send(xs.at[k, rows_of(g * own, own)], back.at[k, chunk, pl.ds(0, own)],
             halo_send.at[k, c], back_recv.at[k, chunk], s, lax.rem(m + far // granules + over, n_tm))
        g, chunk, over = place(2 * n_series - far_in + 1, far_in - 1)
        send(xs.at[k, rows_of(g * own, 8)], back.at[k, chunk, pl.ds(own, 8)],
             halo_send.at[k, c], back_recv.at[k, chunk], s, lax.rem(m + far // granules + over, n_tm))
        g, chunk, over = place(far_in, granules - far_in)
        send(xs.at[k, rows_of(g * own, own)], ahead.at[k, chunk, pl.ds(8, own)],
             halo_send.at[k, c], ahead_recv.at[k, chunk], s,
             lax.rem(m + n_tm - far // granules - 1 + over, n_tm))
        g, chunk, over = place(far_in - 1, granules - far_in + 1)
        send(xs.at[k, rows_of(g * own + own - 8, 8)], ahead.at[k, chunk, pl.ds(0, 8)],
             halo_send.at[k, c], ahead_recv.at[k, chunk], s,
             lax.rem(m + n_tm - far // granules - 1 + over, n_tm))

    def edges_out(k):
        send(xs.at[k, pl.ds(minutes - 8, 8)], edge_before.at[k],
             halo_send.at[k, CHUNKS], edge_recv.at[k, 0], s, lax.rem(m + 1, n_tm))
        send(xs.at[k, pl.ds(0, 8)], edge_after.at[k],
             halo_send.at[k, CHUNKS + 1], edge_recv.at[k, 1], s, lax.rem(m + n_tm - 1, n_tm))

    def halo_wait(k):
        for c in range(CHUNKS):
            wait_for(back.at[k, pl.ds(0, 2)], halo_send.at[k, c])
        wait_for(edge_before.at[k], halo_send.at[k, CHUNKS])
        wait_for(edge_after.at[k], halo_send.at[k, CHUNKS + 1])

    def round_times(k, c):
        at = rows_of(c * cols, cols)
        xb[at] = xs[k, at].astype(BF16)

    def round_loads(o, e):
        at = rows_of(e * series_rows, series_rows)
        block = fs[o, at]
        fb[at] = block.astype(BF16)
        fbt[:, at] = block.T.astype(BF16)

    def gradient(k, c):
        at = rows_of(c * cols, cols)
        x_block = xb[at]
        step = 256
        for i in range(series // step):
            part = pl.ds(i * step, step)
            prod = lax.dot_general(fb[part], x_block, NT, preferred_element_type=F32)
            resid[part] = (prod - obs[part, at].astype(F32)).astype(BF16) * mask[part, at]
        grad = jnp.dot(fbt[...], resid[...], preferred_element_type=F32)
        gs[k, at] = grad.T
        for d in range(1, n_series):
            to = lax.rem(s + d, n_series)
            send(gs.at[k, rows_of((c * n_series + to) * own, own)], got_g.at[k, c, n_series - 1 - d],
                 g_send.at[k, c], g_recv.at[k, c], to, m)

    def smoothing(k, c):
        wait_for(back.at[k, c], back_recv.at[k, c])
        wait_for(ahead.at[k, c], ahead_recv.at[k, c])
        j = c * n_series + s
        first = j * own
        before = xs[k, rows_of(jnp.maximum(first - 8, 0), 8)]
        after = xs[k, rows_of(jnp.minimum(first + own, minutes - 8), 8)]
        window[0:8] = jnp.where(j == 0, edge_before[k], before)
        x = xs[k, rows_of(first, own)]
        window[8:8 + own] = x
        window[8 + own:16 + own] = jnp.where(j == granules - 1, edge_after[k], after)
        t = m * minutes + first + lax.broadcasted_iota(jnp.int32, (own, rank), 0)
        w0 = weights[0:1]
        w1 = weights[1:2]
        prev = jnp.where(t >= 1, window[7:7 + own], 0.0)
        after_one = window[9:9 + own]
        back_far = jnp.where(t >= LAG, back[k, c, 0:own], 0.0)
        back_near = jnp.where(t >= LAG - 1, back[k, c, 1:1 + own], 0.0)
        here = x - w0 * prev - w1 * back_far
        one = jnp.where(t + 1 < total_minutes, after_one - w0 * x - w1 * back_near, 0.0)
        there = jnp.where(
            t + LAG < total_minutes, ahead[k, c, 8:8 + own] - w0 * ahead[k, c, 7:7 + own] - w1 * x, 0.0
        )
        return x, smooth * (here - w0 * one - w1 * there)

    def update_times(k, c):
        x, smooth_grad = smoothing(k, c)
        wait_for(got_g.at[k, c], g_recv.at[k, c])
        at = rows_of((c * n_series + s) * own, own)
        total = gs[k, at]
        for d in range(n_series - 1):
            total = total + got_g[k, c, d]
        xs[k + 1, at] = x - step_time * (total + smooth_grad)
        for d in range(1, n_series):
            send(xs.at[k + 1, at], xs.at[k + 1, at], x_send.at[k, c], x_recv.at[k, c],
                 lax.rem(s + d, n_series), m)
        wait_for(got_g.at[k, c], g_send.at[k, c])

    def times_arrived(k, c):
        wait_for(got_g.at[k, c], x_recv.at[k, c])
        wait_for(got_g.at[k, c], x_send.at[k, c])

    def each(body):
        def step(i, carry):
            body(i)
            return carry
        lax.fori_loop(0, CHUNKS, step, 0)

    def load_gradient(o, e):
        at = rows_of(e * series_rows, series_rows)
        f_block = fb[at]
        step = 256
        for i in range(minutes // step):
            part = pl.ds(i * step, step)
            prod = lax.dot_general(f_block, xb[part], NT, preferred_element_type=F32)
            resid_f[:, part] = (prod - obs[at, part].astype(F32)).astype(BF16) * mask[at, part]
        hs[o, at] = jnp.dot(resid_f[...], xb[...], preferred_element_type=F32)
        send(hs.at[o, rows_of(e * series_rows + half * (1 - core), half)], core_h.at[o, e],
             core_send.at[o, e], core_recv.at[o, e], s, partner)

    def load_share(o, e):
        wait_for(core_h.at[o, e], core_recv.at[o, e])
        sum_h[o, e] = hs[o, rows_of(e * series_rows + half * core, half)] + core_h[o, e]
        for d in range(1, n_pair):
            to = lax.rem(pair + d, n_pair)
            send(sum_h.at[o, e, rows_of(to * own_f, own_f)], got_h.at[o, e, n_pair - 1 - d],
                 h_send.at[o, e], h_recv.at[o, e], s, 2 * to + core)

    def update_loads(o, e):
        wait_for(got_h.at[o, e], h_recv.at[o, e])
        total = sum_h[o, e, rows_of(pair * own_f, own_f)]
        for d in range(n_pair - 1):
            total = total + got_h[o, e, d]
        at = rows_of(e * series_rows + half * core + pair * own_f, own_f)
        f = fs[o, at]
        fs[o + 1, at] = f - step_load * (total + shrink * f)
        for d in range(1, n_pair):
            send(fs.at[o + 1, at], fs.at[o + 1, at], f_send.at[o, e], f_recv.at[o, e],
                 s, 2 * lax.rem(pair + d, n_pair) + core)
        wait_for(core_h.at[o, e], core_send.at[o, e])
        wait_for(got_h.at[o, e], h_send.at[o, e])

    def loads_half(o, e):
        wait_for(got_h.at[o, e], f_recv.at[o, e])
        at = rows_of(e * series_rows + half * core, half)
        send(fs.at[o + 1, at], fs.at[o + 1, at], pair_send.at[o, e], pair_recv.at[o, e], s, partner)
        wait_for(got_h.at[o, e], f_send.at[o, e])

    def loads_arrived(o, e):
        wait_for(core_h.at[o, e], pair_recv.at[o, e])
        wait_for(core_h.at[o, e], pair_send.at[o, e])

    times_in.wait()
    loads_in.wait()
    for c in range(CHUNKS):
        round_times(0, c)
    pl.semaphore_wait(barrier, greetings)
    each(lambda c: halo_out(0, c))
    edges_out(0)
    each(lambda e: round_loads(0, e))

    def outer(o, carry):
        for i in range(TIME_STEPS):
            k = TIME_STEPS * o + i

            def first_half(c, k=k, i=i):
                if i == 0:
                    @pl.when(o == 0)
                    def _():
                        for which in range(2):
                            tile_in(c, which).wait()
                else:
                    times_arrived(k - 1, c)
                    halo_out(k, c)
                    round_times(k, c)
                gradient(k, c)

            each(first_half)
            if i > 0:
                edges_out(k)
            for which, ref in enumerate((edge_before, edge_after)):
                wait_for(ref.at[k], edge_recv.at[k, which])
            each(functools.partial(update_times, k))
            halo_wait(k)

        def settle(c):
            times_arrived(k, c)
            round_times(k + 1, c)

            @pl.when(o < OUTER - 1)
            def _():
                halo_out(k + 1, c)

        each(settle)

        @pl.when(o < OUTER - 1)
        def _():
            edges_out(k + 1)

        def load_first(e):
            load_gradient(o, e)

            @pl.when(e > 0)
            def _():
                load_share(o, e - 1)

        each(load_first)
        load_share(o, CHUNKS - 1)
        each(functools.partial(update_loads, o))
        each(functools.partial(loads_half, o))

        def load_last(e):
            loads_arrived(o, e)

            @pl.when(o < OUTER - 1)
            def _():
                round_loads(o + 1, e)

        each(load_last)
        return carry

    lax.fori_loop(0, OUTER, outer, 0)
    times_back = pltpu.make_async_copy(xs.at[STEPS], times_out, out_sem.at[0])
    loads_back = pltpu.make_async_copy(fs.at[OUTER], loads_out, out_sem.at[1])
    times_back.start()
    loads_back.start()
    times_back.wait()
    loads_back.wait()


def body(observed, mask, loadings, factors, lag_weights):
    n_series, n_tm = lax.axis_size("series"), lax.axis_size("tm")
    series, minutes = observed.shape
    rank = loadings.shape[1]
    cols = minutes // CHUNKS
    own = cols // n_series
    n_pair = n_tm // 2
    series_rows = series // CHUNKS
    half = series_rows // 2
    own_f = half // n_pair
    vmem = pltpu.VMEM
    dma = pltpu.SemaphoreType.DMA
    anywhere = pl.BlockSpec(memory_space=pl.ANY)
    scratch = [
        vmem((series, minutes), BF16),
        vmem((series, minutes), BF16),
        vmem((OUTER + 1, series, rank), F32),
        vmem((STEPS + 1, minutes, rank), F32),
        vmem((STEPS, minutes, rank), F32),
        vmem((OUTER, series, rank), F32),
        vmem((STEPS, CHUNKS, n_series - 1, own, rank), F32),
        vmem((OUTER, CHUNKS, n_pair - 1, own_f, rank), F32),
        vmem((OUTER, CHUNKS, half, rank), F32),
        vmem((OUTER, CHUNKS, half, rank), F32),
        vmem((STEPS, CHUNKS, own + 8, rank), F32),
        vmem((STEPS, CHUNKS, own + 8, rank), F32),
        vmem((STEPS, 8, rank), F32),
        vmem((STEPS, 8, rank), F32),
        vmem((series, rank), BF16),
        vmem((rank, series), BF16),
        vmem((minutes, rank), BF16),
        vmem((series, cols), BF16),
        vmem((series_rows, minutes), BF16),
        vmem((own + 16, rank), F32),
        dma((2,)), dma((2, CHUNKS)), dma((2,)),
        dma((STEPS, CHUNKS)), dma((STEPS, CHUNKS)), dma((STEPS, CHUNKS)), dma((STEPS, CHUNKS)),
        dma((STEPS, CHUNKS + 2)), dma((STEPS, CHUNKS)), dma((STEPS, CHUNKS)), dma((STEPS, 2)),
        dma((OUTER, CHUNKS)), dma((OUTER, CHUNKS)), dma((OUTER, CHUNKS)), dma((OUTER, CHUNKS)),
        dma((OUTER, CHUNKS)), dma((OUTER, CHUNKS)), dma((OUTER, CHUNKS)), dma((OUTER, CHUNKS)),
    ]
    return pl.pallas_call(
        functools.partial(kernel, (n_series, n_tm), (series, minutes)),
        out_shape=(
            jax.ShapeDtypeStruct(loadings.shape, F32),
            jax.ShapeDtypeStruct(factors.shape, F32),
        ),
        in_specs=[anywhere, anywhere, anywhere, anywhere, pl.BlockSpec(memory_space=vmem)],
        out_specs=(anywhere, anywhere),
        scratch_shapes=scratch,
        compiler_params=pltpu.CompilerParams(
            collective_id=0, has_side_effects=True, vmem_limit_bytes=60 * 1024 * 1024
        ),
        name="factorize",
    )(observed, mask, loadings, factors, lag_weights)


def solution(mesh):
    in_specs = (P("series", "tm"), P("series", "tm"), P("series", None), P("tm", None), P())
    out_specs = (P("series", None), P("tm", None))
    return jax.shard_map(body, mesh=mesh, in_specs=in_specs, out_specs=out_specs, check_vma=False)
```

```python
import functools

import jax
import jax.numpy as jnp
from jax import lax
from jax.experimental import pallas as pl
from jax.experimental.pallas import tpu as pltpu
from jax.sharding import PartitionSpec as P

LAG = 1440
OUTER = 2
TIME_STEPS = 2
STEPS = OUTER * TIME_STEPS
CHUNKS = 4
LOAD_CHUNKS = 8

smooth = 4.0
shrink = 0.1
margin = 32.0

MESH = pl.DeviceIdType.MESH
F32 = jnp.float32
BF16 = jnp.bfloat16
NT = (((1,), (1,)), ((), ()))


def rows_of(start, size):
    return pl.ds(pl.multiple_of(start, size), size)


def kernel(
    groups, spans,
    obs_hbm, mask_hbm, loads_hbm, times_hbm, weights_hbm,
    loads_out, times_out,
    obs, mask, weights, fs, xs, gs, hs, got_g, core_h, core_sum, near_h, near_sum, got_h,
    back, ahead, edge_before, edge_after,
    fb, fbt, xb, resid, resid_f, window,
    in_sem, tile_sem,
    g_send, g_recv, x_send, x_recv,
    halo_send, back_recv, ahead_recv, edge_recv,
    core_send, core_recv, near_send, near_recv, h_send, h_recv, f_send, f_recv,
    near_f_send, near_f_recv, core_f_send, core_f_recv,
):
    n_series, n_tm = groups
    series, minutes = spans
    rank = weights.shape[1]
    n_ring = n_tm // 4
    n_x = 2
    n_y = n_series // n_x
    series_offsets = sorted(
        [(dy, dx) for dx in range(n_x) for dy in range(n_y) if dy or dx],
        key=lambda at: -min(at[0], n_y - at[0]) - 2 * at[1],
    )
    ring_offsets = sorted(range(1, n_ring), key=lambda d: -min(d, n_ring - d))
    cols = minutes // CHUNKS
    own = cols // n_series
    granules = minutes // own
    far = LAG // own
    far_in = far % granules
    series_rows = series // LOAD_CHUNKS
    half = series_rows // 2
    quarter = half // 2
    own_f = quarter // n_ring
    total_minutes = minutes * n_tm
    step_time = 1.0 / (series * n_series / rank + margin)
    step_load = 1.0 / total_minutes

    s = lax.axis_index("series")
    m = lax.axis_index("tm")
    core = lax.rem(m, 2)
    near = lax.rem(m // 2, 2)
    ring = m // 4
    core_peer = m + 1 - 2 * core
    near_peer = m + 2 - 4 * near

    def series_peer(dy, dx):
        return n_y * lax.rem(s // n_y + dx, n_x) + lax.rem(s + dy, n_y)

    def ring_peer(d):
        return 4 * lax.rem(ring + d, n_ring) + 2 * near + core

    def send(src, dst, send_sem, recv_sem, to_s, to_m):
        pltpu.make_async_remote_copy(
            src_ref=src, dst_ref=dst, send_sem=send_sem, recv_sem=recv_sem,
            device_id=(to_s, to_m), device_id_type=MESH,
        ).start()

    def wait_for(ref, sem):
        pltpu.make_async_copy(ref, ref, sem).wait()

    barrier = pltpu.get_barrier_semaphore()

    def greet(to_s, to_m):
        pl.semaphore_signal(barrier, inc=1, device_id=(to_s, to_m), device_id_type=MESH)

    for offset in series_offsets:
        greet(series_peer(*offset), m)
    for d in ring_offsets:
        greet(s, ring_peer(d))
    greet(s, core_peer)
    greet(s, near_peer)
    for d in (1, 2):
        greet(s, lax.rem(m + d, n_tm))
        greet(s, lax.rem(m + n_tm - d, n_tm))
    greetings = (n_series - 1) + (n_ring - 1) + 6

    times_in = pltpu.make_async_copy(times_hbm, xs.at[0], in_sem.at[0])
    loads_in = pltpu.make_async_copy(loads_hbm, fs.at[0], in_sem.at[1])
    weights_in = pltpu.make_async_copy(weights_hbm, weights, in_sem.at[2])
    times_in.start()
    loads_in.start()
    weights_in.start()

    def tile_in(c, which):
        ref, hbm = ((obs, obs_hbm), (mask, mask_hbm))[which]
        at = rows_of(c * cols, cols)
        return pltpu.make_async_copy(hbm.at[:, at], ref.at[:, at], tile_sem.at[which, c])

    for c in range(CHUNKS):
        tile_in(c, 0).start()
        tile_in(c, 1).start()

    def halo_out(k, c):
        def place(offset, shift):
            g = c * n_series + lax.rem(s + offset, n_series)
            j = lax.rem(g + shift, granules)
            return g, j // n_series, (g + shift) // granules

        g, chunk, over = place(2 * n_series - far_in, far_in)
        send(xs.at[k, rows_of(g * own, own)], back.at[k, chunk, pl.ds(0, own)],
             halo_send.at[k, c], back_recv.at[k, chunk], s, lax.rem(m + far // granules + over, n_tm))
        g, chunk, over = place(2 * n_series - far_in + 1, far_in - 1)
        send(xs.at[k, rows_of(g * own, 8)], back.at[k, chunk, pl.ds(own, 8)],
             halo_send.at[k, c], back_recv.at[k, chunk], s, lax.rem(m + far // granules + over, n_tm))
        g, chunk, over = place(far_in, granules - far_in)
        send(xs.at[k, rows_of(g * own, own)], ahead.at[k, chunk, pl.ds(8, own)],
             halo_send.at[k, c], ahead_recv.at[k, chunk], s,
             lax.rem(m + n_tm - far // granules - 1 + over, n_tm))
        g, chunk, over = place(far_in - 1, granules - far_in + 1)
        send(xs.at[k, rows_of(g * own + own - 8, 8)], ahead.at[k, chunk, pl.ds(0, 8)],
             halo_send.at[k, c], ahead_recv.at[k, chunk], s,
             lax.rem(m + n_tm - far // granules - 1 + over, n_tm))

    def edges_out(k):
        send(xs.at[k, pl.ds(minutes - 8, 8)], edge_before.at[k],
             halo_send.at[k, CHUNKS], edge_recv.at[k, 0], s, lax.rem(m + 1, n_tm))
        send(xs.at[k, pl.ds(0, 8)], edge_after.at[k],
             halo_send.at[k, CHUNKS + 1], edge_recv.at[k, 1], s, lax.rem(m + n_tm - 1, n_tm))

    def halo_wait(k):
        for c in range(CHUNKS):
            wait_for(back.at[k, pl.ds(0, 2)], halo_send.at[k, c])
        wait_for(edge_before.at[k], halo_send.at[k, CHUNKS])
        wait_for(edge_after.at[k], halo_send.at[k, CHUNKS + 1])

    def round_times(k, c):
        at = rows_of(c * cols, cols)
        xb[at] = xs[k, at].astype(BF16)

    def round_loads(o, e):
        at = rows_of(e * series_rows, series_rows)
        block = fs[o, at]
        fb[at] = block.astype(BF16)
        fbt[:, at] = block.T.astype(BF16)

    def gradient(k, c):
        at = rows_of(c * cols, cols)
        x_block = xb[at]
        step = 256
        for i in range(series // step):
            part = pl.ds(i * step, step)
            prod = lax.dot_general(fb[part], x_block, NT, preferred_element_type=F32)
            resid[part] = (prod - obs[part, at].astype(F32)).astype(BF16) * mask[part, at]
        grad = jnp.dot(fbt[...], resid[...], preferred_element_type=F32)
        gs[k, at] = grad.T

    def share_gradient(k, c):
        for slot, offset in enumerate(series_offsets):
            to = series_peer(*offset)
            send(gs.at[k, rows_of((c * n_series + to) * own, own)], got_g.at[k, c, slot],
                 g_send.at[k, c], g_recv.at[k, c], to, m)

    def smoothing(k, c):
        wait_for(back.at[k, c], back_recv.at[k, c])
        wait_for(ahead.at[k, c], ahead_recv.at[k, c])
        j = c * n_series + s
        first = j * own
        before = xs[k, rows_of(jnp.maximum(first - 8, 0), 8)]
        after = xs[k, rows_of(jnp.minimum(first + own, minutes - 8), 8)]
        window[0:8] = jnp.where(j == 0, edge_before[k], before)
        x = xs[k, rows_of(first, own)]
        window[8:8 + own] = x
        window[8 + own:16 + own] = jnp.where(j == granules - 1, edge_after[k], after)
        t = m * minutes + first + lax.broadcasted_iota(jnp.int32, (own, rank), 0)
        w0 = weights[0:1]
        w1 = weights[1:2]
        prev = jnp.where(t >= 1, window[7:7 + own], 0.0)
        after_one = window[9:9 + own]
        back_far = jnp.where(t >= LAG, back[k, c, 0:own], 0.0)
        back_near = jnp.where(t >= LAG - 1, back[k, c, 1:1 + own], 0.0)
        here = x - w0 * prev - w1 * back_far
        one = jnp.where(t + 1 < total_minutes, after_one - w0 * x - w1 * back_near, 0.0)
        there = jnp.where(
            t + LAG < total_minutes, ahead[k, c, 8:8 + own] - w0 * ahead[k, c, 7:7 + own] - w1 * x, 0.0
        )
        return x, smooth * (here - w0 * one - w1 * there)

    def update_times(k, c):
        x, smooth_grad = smoothing(k, c)
        wait_for(got_g.at[k, c], g_recv.at[k, c])
        at = rows_of((c * n_series + s) * own, own)
        total = gs[k, at]
        for d in range(n_series - 1):
            total = total + got_g[k, c, d]
        xs[k + 1, at] = x - step_time * (total + smooth_grad)
        for offset in series_offsets:
            send(xs.at[k + 1, at], xs.at[k + 1, at], x_send.at[k, c], x_recv.at[k, c],
                 series_peer(*offset), m)
        wait_for(got_g.at[k, c], g_send.at[k, c])

    def times_arrived(k, c):
        wait_for(got_g.at[k, c], x_recv.at[k, c])
        wait_for(got_g.at[k, c], x_send.at[k, c])

    def each(body, count=CHUNKS):
        def step(i, carry):
            body(i)
            return carry
        lax.fori_loop(0, count, step, 0)

    def load_gradient(o, e):
        at = rows_of(e * series_rows, series_rows)
        f_block = fb[at]
        step = 256
        for i in range(minutes // step):
            part = pl.ds(i * step, step)
            prod = lax.dot_general(f_block, xb[part], NT, preferred_element_type=F32)
            resid_f[:, part] = (prod - obs[at, part].astype(F32)).astype(BF16) * mask[at, part]
        hs[o, at] = jnp.dot(resid_f[...], xb[...], preferred_element_type=F32)
        send(hs.at[o, rows_of(e * series_rows + half * (1 - core), half)], core_h.at[o, e],
             core_send.at[o, e], core_recv.at[o, e], s, core_peer)

    def core_share(o, e):
        wait_for(core_h.at[o, e], core_recv.at[o, e])
        core_sum[o, e] = hs[o, rows_of(e * series_rows + half * core, half)] + core_h[o, e]
        send(core_sum.at[o, e, rows_of(quarter * (1 - near), quarter)], near_h.at[o, e],
             near_send.at[o, e], near_recv.at[o, e], s, near_peer)

    def near_share(o, e):
        wait_for(near_h.at[o, e], near_recv.at[o, e])
        near_sum[o, e] = core_sum[o, e, rows_of(quarter * near, quarter)] + near_h[o, e]
        for slot, d in enumerate(ring_offsets):
            to = lax.rem(ring + d, n_ring)
            send(near_sum.at[o, e, rows_of(to * own_f, own_f)], got_h.at[o, e, slot],
                 h_send.at[o, e], h_recv.at[o, e], s, ring_peer(d))

    def quarter_at(e):
        return e * series_rows + half * core + quarter * near

    def update_loads(o, e):
        wait_for(got_h.at[o, e], h_recv.at[o, e])
        total = near_sum[o, e, rows_of(ring * own_f, own_f)]
        for d in range(n_ring - 1):
            total = total + got_h[o, e, d]
        at = rows_of(quarter_at(e) + ring * own_f, own_f)
        f = fs[o, at]
        fs[o + 1, at] = f - step_load * (total + shrink * f)
        for d in ring_offsets:
            send(fs.at[o + 1, at], fs.at[o + 1, at], f_send.at[o, e], f_recv.at[o, e], s, ring_peer(d))
        wait_for(core_h.at[o, e], core_send.at[o, e])
        wait_for(near_h.at[o, e], near_send.at[o, e])
        wait_for(got_h.at[o, e], h_send.at[o, e])

    def quarter_out(o, e):
        wait_for(got_h.at[o, e], f_recv.at[o, e])
        at = rows_of(quarter_at(e), quarter)
        send(fs.at[o + 1, at], fs.at[o + 1, at], near_f_send.at[o, e], near_f_recv.at[o, e], s, near_peer)
        wait_for(got_h.at[o, e], f_send.at[o, e])

    def half_out(o, e):
        wait_for(near_h.at[o, e], near_f_recv.at[o, e])
        at = rows_of(e * series_rows + half * core, half)
        send(fs.at[o + 1, at], fs.at[o + 1, at], core_f_send.at[o, e], core_f_recv.at[o, e], s, core_peer)
        wait_for(near_h.at[o, e], near_f_send.at[o, e])

    def loads_arrived(o, e):
        wait_for(core_h.at[o, e], core_f_recv.at[o, e])
        wait_for(core_h.at[o, e], core_f_send.at[o, e])

    times_in.wait()
    loads_in.wait()
    weights_in.wait()
    for c in range(CHUNKS):
        round_times(0, c)
    each(functools.partial(round_loads, 0), LOAD_CHUNKS)
    for which in range(2):
        tile_in(0, which).wait()
    gradient(0, 0)
    pl.semaphore_wait(barrier, greetings)

    def outer(o, carry):
        for i in range(TIME_STEPS):
            k = TIME_STEPS * o + i

            def first_half(c, k=k, i=i):
                if i == 0:
                    @pl.when(jnp.logical_and(o == 0, c > 0))
                    def _():
                        for which in range(2):
                            tile_in(c, which).wait()

                    @pl.when(o + c > 0)
                    def _():
                        gradient(k, c)
                else:
                    times_arrived(k - 1, c)
                    halo_out(k, c)
                    round_times(k, c)
                    gradient(k, c)
                share_gradient(k, c)
                if i == 0:
                    @pl.when(o == 0)
                    def _():
                        halo_out(0, lax.rem(c + CHUNKS // 2, CHUNKS))

            each(first_half)
            if i > 0:
                edges_out(k)
            else:
                @pl.when(o == 0)
                def _():
                    edges_out(0)

            for which, ref in enumerate((edge_before, edge_after)):
                wait_for(ref.at[k], edge_recv.at[k, which])
            each(functools.partial(update_times, k))
            halo_wait(k)

        def settle(c):
            times_arrived(k, c)
            round_times(k + 1, c)

            @pl.when(o < OUTER - 1)
            def _():
                halo_out(k + 1, c)

        each(settle)

        @pl.when(o < OUTER - 1)
        def _():
            edges_out(k + 1)

        lag = 4

        def load_first(e):
            load_gradient(o, e)

            @pl.when(e >= lag)
            def _():
                core_share(o, e - lag)

        each(load_first, LOAD_CHUNKS)
        each(lambda e: core_share(o, e + LOAD_CHUNKS - lag), lag)

        @pl.when(o == OUTER - 1)
        def _():
            times_out[...] = xs[STEPS]

        each(functools.partial(near_share, o), LOAD_CHUNKS)
        each(functools.partial(update_loads, o), LOAD_CHUNKS)
        def load_back(e):
            quarter_out(o, e)

            @pl.when(e >= lag)
            def _():
                half_out(o, e - lag)

        each(load_back, LOAD_CHUNKS)
        each(lambda e: half_out(o, e + LOAD_CHUNKS - lag), lag)

        def load_last(e):
            loads_arrived(o, e)

            @pl.when(o < OUTER - 1)
            def _():
                round_loads(o + 1, e)

            @pl.when(o == OUTER - 1)
            def _():
                at = rows_of(e * series_rows, series_rows)
                loads_out[at] = fs[OUTER, at]

        each(load_last, LOAD_CHUNKS)
        return carry

    lax.fori_loop(0, OUTER, outer, 0)


def body(observed, mask, loadings, factors, lag_weights):
    n_series, n_tm = lax.axis_size("series"), lax.axis_size("tm")
    series, minutes = observed.shape
    rank = loadings.shape[1]
    cols = minutes // CHUNKS
    own = cols // n_series
    n_ring = n_tm // 4
    half = series // LOAD_CHUNKS // 2
    quarter = half // 2
    own_f = quarter // n_ring
    arguments = (observed, mask, loadings, factors, lag_weights)
    vmem = pltpu.VMEM
    dma = pltpu.SemaphoreType.DMA
    hbm = pl.BlockSpec(memory_space=pltpu.HBM)
    whole = pl.BlockSpec(memory_space=vmem)
    scratch = [
        vmem((series, minutes), BF16),
        vmem((series, minutes), BF16),
        vmem(lag_weights.shape, F32),
        vmem((OUTER + 1, series, rank), F32),
        vmem((STEPS + 1, minutes, rank), F32),
        vmem((STEPS, minutes, rank), F32),
        vmem((OUTER, series, rank), F32),
        vmem((STEPS, CHUNKS, n_series - 1, own, rank), F32),
        vmem((OUTER, LOAD_CHUNKS, half, rank), F32),
        vmem((OUTER, LOAD_CHUNKS, half, rank), F32),
        vmem((OUTER, LOAD_CHUNKS, quarter, rank), F32),
        vmem((OUTER, LOAD_CHUNKS, quarter, rank), F32),
        vmem((OUTER, LOAD_CHUNKS, n_ring - 1, own_f, rank), F32),
        vmem((STEPS, CHUNKS, own + 8, rank), F32),
        vmem((STEPS, CHUNKS, own + 8, rank), F32),
        vmem((STEPS, 8, rank), F32),
        vmem((STEPS, 8, rank), F32),
        vmem((series, rank), BF16),
        vmem((rank, series), BF16),
        vmem((minutes, rank), BF16),
        vmem((series, cols), BF16),
        vmem((series // LOAD_CHUNKS, minutes), BF16),
        vmem((own + 16, rank), F32),
        dma((3,)), dma((2, CHUNKS)),
        dma((STEPS, CHUNKS)), dma((STEPS, CHUNKS)), dma((STEPS, CHUNKS)), dma((STEPS, CHUNKS)),
        dma((STEPS, CHUNKS + 2)), dma((STEPS, CHUNKS)), dma((STEPS, CHUNKS)), dma((STEPS, 2)),
    ] + [dma((OUTER, LOAD_CHUNKS))] * 12
    return pl.pallas_call(
        functools.partial(kernel, (n_series, n_tm), (series, minutes)),
        out_shape=(
            jax.ShapeDtypeStruct(loadings.shape, F32),
            jax.ShapeDtypeStruct(factors.shape, F32),
        ),
        in_specs=[hbm] * len(arguments),
        out_specs=(whole, whole),
        scratch_shapes=scratch,
        compiler_params=pltpu.CompilerParams(
            collective_id=0, has_side_effects=True, vmem_limit_bytes=50 * 1024 * 1024
        ),
        name="factorize",
    )(*(pltpu.with_memory_space_constraint(x, pltpu.HBM) for x in arguments))


def solution(mesh):
    in_specs = (P("series", "tm"), P("series", "tm"), P("series", None), P("tm", None), P())
    out_specs = (P("series", None), P("tm", None))
    return jax.shard_map(body, mesh=mesh, in_specs=in_specs, out_specs=out_specs, check_vma=False)
```

```python
import functools

import jax
import jax.numpy as jnp
from jax import lax
from jax.experimental import pallas as pl
from jax.experimental.pallas import tpu as pltpu
from jax.sharding import PartitionSpec as P

LAG = 1440
OUTER = 2
TIME_STEPS = 2
STEPS = OUTER * TIME_STEPS
CHUNKS = 4
LOAD_CHUNKS = 8
LOAD_GROUP = 4

smooth = 4.0
shrink = 0.1
margin = 32.0

MESH = pl.DeviceIdType.MESH
F32 = jnp.float32
BF16 = jnp.bfloat16
NT = (((1,), (1,)), ((), ()))


def rows_of(start, size):
    return pl.ds(pl.multiple_of(start, size), size)


def kernel(
    groups, spans,
    obs_hbm, mask_hbm, loads_hbm, times_hbm, weights_hbm,
    loads_out, times_out,
    obs, mask, weights, fs, xs, gs, hs, got_g, core_h, core_sum, near_h, near_sum, got_h,
    back, ahead, edge_before, edge_after,
    fb, fbt, xb, resid, window,
    in_sem, tile_sem,
    g_send, g_recv, x_send, x_recv,
    halo_send, back_recv, ahead_recv, edge_recv,
    core_send, core_recv, near_send, near_recv, h_send, h_recv, f_send, f_recv,
    near_f_send, near_f_recv, core_f_send, core_f_recv,
):
    n_series, n_tm = groups
    series, minutes = spans
    rank = weights.shape[1]
    n_ring = n_tm // 4
    n_x = 2
    n_y = n_series // n_x
    series_offsets = sorted(
        [(dy, dx) for dx in range(n_x) for dy in range(n_y) if dy or dx],
        key=lambda at: -min(at[0], n_y - at[0]) - 2 * at[1],
    )
    ring_offsets = sorted(range(1, n_ring), key=lambda d: -min(d, n_ring - d))
    cols = minutes // CHUNKS
    own = cols // n_series
    granules = minutes // own
    far = LAG // own
    far_in = far % granules
    series_rows = series // LOAD_CHUNKS
    half = series_rows // 2
    quarter = half // 2
    own_f = quarter // n_ring
    total_minutes = minutes * n_tm
    step_time = 1.0 / (series * n_series / rank + margin)
    step_load = 1.0 / total_minutes

    s = lax.axis_index("series")
    m = lax.axis_index("tm")
    core = lax.rem(m, 2)
    near = lax.rem(m // 2, 2)
    ring = m // 4
    core_peer = m + 1 - 2 * core
    near_peer = m + 2 - 4 * near

    def series_peer(dy, dx):
        return n_y * lax.rem(s // n_y + dx, n_x) + lax.rem(s + dy, n_y)

    def ring_peer(d):
        return 4 * lax.rem(ring + d, n_ring) + 2 * near + core

    def send(src, dst, send_sem, recv_sem, to_s, to_m):
        pltpu.make_async_remote_copy(
            src_ref=src, dst_ref=dst, send_sem=send_sem, recv_sem=recv_sem,
            device_id=(to_s, to_m), device_id_type=MESH,
        ).start()

    def wait_for(ref, sem):
        pltpu.make_async_copy(ref, ref, sem).wait()

    barrier = pltpu.get_barrier_semaphore()

    def greet(to_s, to_m):
        pl.semaphore_signal(barrier, inc=1, device_id=(to_s, to_m), device_id_type=MESH)

    for offset in series_offsets:
        greet(series_peer(*offset), m)
    for d in ring_offsets:
        greet(s, ring_peer(d))
    greet(s, core_peer)
    greet(s, near_peer)
    for d in (1, 2):
        greet(s, lax.rem(m + d, n_tm))
        greet(s, lax.rem(m + n_tm - d, n_tm))
    greetings = (n_series - 1) + (n_ring - 1) + 6

    times_in = pltpu.make_async_copy(times_hbm, xs.at[0], in_sem.at[0])
    loads_in = pltpu.make_async_copy(loads_hbm, fs.at[0], in_sem.at[1])
    weights_in = pltpu.make_async_copy(weights_hbm, weights, in_sem.at[2])
    times_in.start()
    loads_in.start()
    weights_in.start()

    def tile_in(c, which):
        ref, hbm = ((obs, obs_hbm), (mask, mask_hbm))[which]
        at = rows_of(c * cols, cols)
        return pltpu.make_async_copy(hbm.at[:, at], ref.at[:, at], tile_sem.at[which, c])

    for c in range(CHUNKS):
        tile_in(c, 0).start()
        tile_in(c, 1).start()

    def halo_out(k, c):
        def place(offset, shift):
            g = c * n_series + lax.rem(s + offset, n_series)
            j = lax.rem(g + shift, granules)
            return g, j // n_series, (g + shift) // granules

        g, chunk, over = place(2 * n_series - far_in, far_in)
        send(xs.at[k, rows_of(g * own, own)], back.at[k, chunk, pl.ds(0, own)],
             halo_send.at[k, c], back_recv.at[k, chunk], s, lax.rem(m + far // granules + over, n_tm))
        g, chunk, over = place(2 * n_series - far_in + 1, far_in - 1)
        send(xs.at[k, rows_of(g * own, 8)], back.at[k, chunk, pl.ds(own, 8)],
             halo_send.at[k, c], back_recv.at[k, chunk], s, lax.rem(m + far // granules + over, n_tm))
        g, chunk, over = place(far_in, granules - far_in)
        send(xs.at[k, rows_of(g * own, own)], ahead.at[k, chunk, pl.ds(8, own)],
             halo_send.at[k, c], ahead_recv.at[k, chunk], s,
             lax.rem(m + n_tm - far // granules - 1 + over, n_tm))
        g, chunk, over = place(far_in - 1, granules - far_in + 1)
        send(xs.at[k, rows_of(g * own + own - 8, 8)], ahead.at[k, chunk, pl.ds(0, 8)],
             halo_send.at[k, c], ahead_recv.at[k, chunk], s,
             lax.rem(m + n_tm - far // granules - 1 + over, n_tm))

    def edges_out(k):
        send(xs.at[k, pl.ds(minutes - 8, 8)], edge_before.at[k],
             halo_send.at[k, CHUNKS], edge_recv.at[k, 0], s, lax.rem(m + 1, n_tm))
        send(xs.at[k, pl.ds(0, 8)], edge_after.at[k],
             halo_send.at[k, CHUNKS + 1], edge_recv.at[k, 1], s, lax.rem(m + n_tm - 1, n_tm))

    def halo_wait(k):
        for c in range(CHUNKS):
            wait_for(back.at[k, pl.ds(0, 2)], halo_send.at[k, c])
        wait_for(edge_before.at[k], halo_send.at[k, CHUNKS])
        wait_for(edge_after.at[k], halo_send.at[k, CHUNKS + 1])

    def round_times(k, c):
        at = rows_of(c * cols, cols)
        xb[at] = xs[k, at].astype(BF16)

    def round_loads(o, e):
        at = rows_of(e * series_rows, series_rows)
        block = fs[o, at]
        fb[at] = block.astype(BF16)
        fbt[:, at] = block.T.astype(BF16)

    def gradient(k, c):
        at = rows_of(c * cols, cols)
        x_block = xb[at]
        step = 256
        for i in range(series // step):
            part = pl.ds(i * step, step)
            prod = lax.dot_general(fb[part], x_block, NT, preferred_element_type=F32)
            resid[part] = (prod - obs[part, at].astype(F32)).astype(BF16) * mask[part, at]
        grad = jnp.dot(fbt[...], resid[...], preferred_element_type=F32)
        gs[k, at] = grad.T

    def share_gradient(k, c):
        for slot, offset in enumerate(series_offsets):
            to = series_peer(*offset)
            send(gs.at[k, rows_of((c * n_series + to) * own, own)], got_g.at[k, c, slot],
                 g_send.at[k, c], g_recv.at[k, c], to, m)

    def smoothing(k, c):
        wait_for(back.at[k, c], back_recv.at[k, c])
        wait_for(ahead.at[k, c], ahead_recv.at[k, c])
        j = c * n_series + s
        first = j * own
        before = xs[k, rows_of(jnp.maximum(first - 8, 0), 8)]
        after = xs[k, rows_of(jnp.minimum(first + own, minutes - 8), 8)]
        window[0:8] = jnp.where(j == 0, edge_before[k], before)
        x = xs[k, rows_of(first, own)]
        window[8:8 + own] = x
        window[8 + own:16 + own] = jnp.where(j == granules - 1, edge_after[k], after)
        t = m * minutes + first + lax.broadcasted_iota(jnp.int32, (own, rank), 0)
        w0 = weights[0:1]
        w1 = weights[1:2]
        prev = jnp.where(t >= 1, window[7:7 + own], 0.0)
        after_one = window[9:9 + own]
        back_far = jnp.where(t >= LAG, back[k, c, 0:own], 0.0)
        back_near = jnp.where(t >= LAG - 1, back[k, c, 1:1 + own], 0.0)
        here = x - w0 * prev - w1 * back_far
        one = jnp.where(t + 1 < total_minutes, after_one - w0 * x - w1 * back_near, 0.0)
        there = jnp.where(
            t + LAG < total_minutes, ahead[k, c, 8:8 + own] - w0 * ahead[k, c, 7:7 + own] - w1 * x, 0.0
        )
        return x, smooth * (here - w0 * one - w1 * there)

    def update_times(k, c):
        x, smooth_grad = smoothing(k, c)
        wait_for(got_g.at[k, c], g_recv.at[k, c])
        at = rows_of((c * n_series + s) * own, own)
        total = gs[k, at]
        for d in range(n_series - 1):
            total = total + got_g[k, c, d]
        xs[k + 1, at] = x - step_time * (total + smooth_grad)
        for offset in series_offsets:
            send(xs.at[k + 1, at], xs.at[k + 1, at], x_send.at[k, c], x_recv.at[k, c],
                 series_peer(*offset), m)
        wait_for(got_g.at[k, c], g_send.at[k, c])

    def times_arrived(k, c):
        wait_for(got_g.at[k, c], x_recv.at[k, c])
        wait_for(got_g.at[k, c], x_send.at[k, c])

    def each(body, count=CHUNKS):
        def step(i, carry):
            body(i)
            return carry
        lax.fori_loop(0, count, step, 0)

    def load_partial(o, c):
        at = rows_of(c * cols, cols)
        x_block = xb[at]
        step = 256
        for i in range(series // step):
            part = pl.ds(i * step, step)
            prod = lax.dot_general(fb[part], x_block, NT, preferred_element_type=F32)
            resid[part] = (prod - obs[part, at].astype(F32)).astype(BF16) * mask[part, at]
        hs[o] += jnp.dot(resid[...], x_block, preferred_element_type=F32)

    def load_gradient(o, pair):
        size = LOAD_GROUP * series_rows
        at = rows_of(pair * size, size)
        last = pl.ds(minutes - cols, cols)
        x_block = xb[last]
        prod = lax.dot_general(fb[at], x_block, NT, preferred_element_type=F32)
        rest = (prod - obs[at, last].astype(F32)).astype(BF16) * mask[at, last]
        hs[o, at] += jnp.dot(rest, x_block, preferred_element_type=F32)
        for i in range(LOAD_GROUP):
            e = pair * LOAD_GROUP + i
            send(hs.at[o, rows_of(e * series_rows + half * (1 - core), half)], core_h.at[o, e],
                 core_send.at[o, e], core_recv.at[o, e], s, core_peer)

    def core_share(o, e):
        wait_for(core_h.at[o, e], core_recv.at[o, e])
        core_sum[o, e] = hs[o, rows_of(e * series_rows + half * core, half)] + core_h[o, e]
        send(core_sum.at[o, e, rows_of(quarter * (1 - near), quarter)], near_h.at[o, e],
             near_send.at[o, e], near_recv.at[o, e], s, near_peer)

    def near_share(o, e):
        wait_for(near_h.at[o, e], near_recv.at[o, e])
        near_sum[o, e] = core_sum[o, e, rows_of(quarter * near, quarter)] + near_h[o, e]
        for slot, d in enumerate(ring_offsets):
            to = lax.rem(ring + d, n_ring)
            send(near_sum.at[o, e, rows_of(to * own_f, own_f)], got_h.at[o, e, slot],
                 h_send.at[o, e], h_recv.at[o, e], s, ring_peer(d))

    def quarter_at(e):
        return e * series_rows + half * core + quarter * near

    def update_loads(o, e):
        wait_for(got_h.at[o, e], h_recv.at[o, e])
        total = near_sum[o, e, rows_of(ring * own_f, own_f)]
        for d in range(n_ring - 1):
            total = total + got_h[o, e, d]
        at = rows_of(quarter_at(e) + ring * own_f, own_f)
        f = fs[o, at]
        fs[o + 1, at] = f - step_load * (total + shrink * f)
        for d in ring_offsets:
            send(fs.at[o + 1, at], fs.at[o + 1, at], f_send.at[o, e], f_recv.at[o, e], s, ring_peer(d))
        wait_for(core_h.at[o, e], core_send.at[o, e])
        wait_for(near_h.at[o, e], near_send.at[o, e])
        wait_for(got_h.at[o, e], h_send.at[o, e])

    def quarter_out(o, e):
        wait_for(got_h.at[o, e], f_recv.at[o, e])
        at = rows_of(quarter_at(e), quarter)
        send(fs.at[o + 1, at], fs.at[o + 1, at], near_f_send.at[o, e], near_f_recv.at[o, e], s, near_peer)
        wait_for(got_h.at[o, e], f_send.at[o, e])

    def half_out(o, e):
        wait_for(near_h.at[o, e], near_f_recv.at[o, e])
        at = rows_of(e * series_rows + half * core, half)
        send(fs.at[o + 1, at], fs.at[o + 1, at], core_f_send.at[o, e], core_f_recv.at[o, e], s, core_peer)
        wait_for(near_h.at[o, e], near_f_send.at[o, e])

    def loads_arrived(o, e):
        wait_for(core_h.at[o, e], core_f_recv.at[o, e])
        wait_for(core_h.at[o, e], core_f_send.at[o, e])

    times_in.wait()
    loads_in.wait()
    weights_in.wait()
    for c in range(CHUNKS):
        round_times(0, c)
    each(functools.partial(round_loads, 0), LOAD_CHUNKS)
    for which in range(2):
        tile_in(0, which).wait()
    gradient(0, 0)
    pl.semaphore_wait(barrier, greetings)

    def outer(o, carry):
        for i in range(TIME_STEPS):
            k = TIME_STEPS * o + i

            def first_half(c, k=k, i=i):
                if i == 0:
                    @pl.when(jnp.logical_and(o == 0, c > 0))
                    def _():
                        for which in range(2):
                            tile_in(c, which).wait()

                    @pl.when(o + c > 0)
                    def _():
                        gradient(k, c)
                else:
                    times_arrived(k - 1, c)
                    halo_out(k, c)
                    round_times(k, c)
                    gradient(k, c)
                share_gradient(k, c)
                if i == 0:
                    @pl.when(o == 0)
                    def _():
                        halo_out(0, lax.rem(c + CHUNKS // 2, CHUNKS))

            each(first_half)
            if i == 0:
                hs[o] = jnp.zeros_like(hs[o])
            if i > 0:
                edges_out(k)
            else:
                @pl.when(o == 0)
                def _():
                    edges_out(0)

            for which, ref in enumerate((edge_before, edge_after)):
                wait_for(ref.at[k], edge_recv.at[k, which])
            each(functools.partial(update_times, k))
            halo_wait(k)

        def settle(c):
            times_arrived(k, c)
            round_times(k + 1, c)

            @pl.when(o < OUTER - 1)
            def _():
                halo_out(k + 1, c)

            @pl.when(c < CHUNKS - 1)
            def _():
                load_partial(o, c)

        each(settle)

        @pl.when(o < OUTER - 1)
        def _():
            edges_out(k + 1)

        lag = 4
        each(functools.partial(load_gradient, o), LOAD_CHUNKS // LOAD_GROUP)
        each(functools.partial(core_share, o), LOAD_CHUNKS)

        @pl.when(o == OUTER - 1)
        def _():
            times_out[...] = xs[STEPS]

        each(functools.partial(near_share, o), LOAD_CHUNKS)
        each(functools.partial(update_loads, o), LOAD_CHUNKS)
        def load_back(e):
            quarter_out(o, e)

            @pl.when(e >= lag)
            def _():
                half_out(o, e - lag)

        each(load_back, LOAD_CHUNKS)
        each(lambda e: half_out(o, e + LOAD_CHUNKS - lag), lag)

        def load_last(e):
            loads_arrived(o, e)

            @pl.when(o < OUTER - 1)
            def _():
                round_loads(o + 1, e)

            @pl.when(o == OUTER - 1)
            def _():
                at = rows_of(e * series_rows, series_rows)
                loads_out[at] = fs[OUTER, at]

        each(load_last, LOAD_CHUNKS)
        return carry

    lax.fori_loop(0, OUTER, outer, 0)


def copy_out(loads, times, loads_hbm, times_hbm, sem):
    copies = [
        pltpu.make_async_copy(loads, loads_hbm, sem.at[0]),
        pltpu.make_async_copy(times, times_hbm, sem.at[1]),
    ]
    for copy in copies:
        copy.start()
    for copy in copies:
        copy.wait()


def body(observed, mask, loadings, factors, lag_weights):
    n_series, n_tm = lax.axis_size("series"), lax.axis_size("tm")
    series, minutes = observed.shape
    rank = loadings.shape[1]
    cols = minutes // CHUNKS
    own = cols // n_series
    n_ring = n_tm // 4
    half = series // LOAD_CHUNKS // 2
    quarter = half // 2
    own_f = quarter // n_ring
    arguments = (observed, mask, loadings, factors, lag_weights)
    vmem = pltpu.VMEM
    dma = pltpu.SemaphoreType.DMA
    hbm = pl.BlockSpec(memory_space=pltpu.HBM)
    whole = pl.BlockSpec(memory_space=vmem)
    scratch = [
        vmem((series, minutes), BF16),
        vmem((series, minutes), BF16),
        vmem(lag_weights.shape, F32),
        vmem((OUTER + 1, series, rank), F32),
        vmem((STEPS + 1, minutes, rank), F32),
        vmem((STEPS, minutes, rank), F32),
        vmem((OUTER, series, rank), F32),
        vmem((STEPS, CHUNKS, n_series - 1, own, rank), F32),
        vmem((OUTER, LOAD_CHUNKS, half, rank), F32),
        vmem((OUTER, LOAD_CHUNKS, half, rank), F32),
        vmem((OUTER, LOAD_CHUNKS, quarter, rank), F32),
        vmem((OUTER, LOAD_CHUNKS, quarter, rank), F32),
        vmem((OUTER, LOAD_CHUNKS, n_ring - 1, own_f, rank), F32),
        vmem((STEPS, CHUNKS, own + 8, rank), F32),
        vmem((STEPS, CHUNKS, own + 8, rank), F32),
        vmem((STEPS, 8, rank), F32),
        vmem((STEPS, 8, rank), F32),
        vmem((series, rank), BF16),
        vmem((rank, series), BF16),
        vmem((minutes, rank), BF16),
        vmem((series, cols), BF16),
        vmem((own + 16, rank), F32),
        dma((3,)), dma((2, CHUNKS)),
        dma((STEPS, CHUNKS)), dma((STEPS, CHUNKS)), dma((STEPS, CHUNKS)), dma((STEPS, CHUNKS)),
        dma((STEPS, CHUNKS + 2)), dma((STEPS, CHUNKS)), dma((STEPS, CHUNKS)), dma((STEPS, 2)),
    ] + [dma((OUTER, LOAD_CHUNKS))] * 12
    loads, times = pl.pallas_call(
        functools.partial(kernel, (n_series, n_tm), (series, minutes)),
        out_shape=(
            jax.ShapeDtypeStruct(loadings.shape, F32),
            jax.ShapeDtypeStruct(factors.shape, F32),
        ),
        in_specs=[hbm] * len(arguments),
        out_specs=(whole, whole),
        scratch_shapes=scratch,
        compiler_params=pltpu.CompilerParams(
            collective_id=0, has_side_effects=True, vmem_limit_bytes=50 * 1024 * 1024
        ),
        name="factorize",
    )(*(pltpu.with_memory_space_constraint(x, pltpu.HBM) for x in arguments))

    return pl.pallas_call(
        copy_out,
        out_shape=(
            jax.ShapeDtypeStruct(loadings.shape, F32),
            jax.ShapeDtypeStruct(factors.shape, F32),
        ),
        in_specs=[whole, whole],
        out_specs=(hbm, hbm),
        scratch_shapes=[dma((2,))],
        compiler_params=pltpu.CompilerParams(vmem_limit_bytes=1024 * 1024),
        name="copy_out",
    )(loads, times)


def solution(mesh):
    in_specs = (P("series", "tm"), P("series", "tm"), P("series", None), P("tm", None), P())
    out_specs = (P("series", None), P("tm", None))
    return jax.shard_map(body, mesh=mesh, in_specs=in_specs, out_specs=out_specs, check_vma=False)
```
